256 devices in a mesh: depth: 16 (over z, core), freq: 16 (over x, y).
Axes of the slice: x: 4, y: 4, z: 8, core: 2. Of those that a mesh axis runs over, the one named last changes fastest.
Arguments:
- fields_top: bfloat16 [16, 2, 16, 2, 384, 384], P('depth', None, 'freq'), may hold values from -6 to 6
- surface: bfloat16 [2, 2, 16, 2, 384, 384], P(None, None, 'freq'), may hold values from -6 to 6
- up_state: bfloat16 [16, 16, 2, 384, 384], P('depth', 'freq'), may hold values from -6 to 6
- angular_freq: float32 [16], P('freq'), may hold values from 0.5 to 2.5
- class_slowness: float32 [8], replicated, may hold values from 0.6 to 1.3
- velocity_class: int32 [16, 12, 12], P('depth'), may hold values from 0 to 7
- slowness_detail: float32 [16, 384, 384], P('depth'), may hold values from 0.5 to 1.5
Outputs:
- reflectivity: bfloat16 [16, 384, 384], P('depth', 'freq')
- up_out: bfloat16 [16, 16, 2, 384, 384], P('depth', 'freq')
The draws below stay inside these ranges and needn't reach their ends.
All inputs are finite; a program needn't handle non-finite values.
Results may differ from the reference program's by a relative error of at most 0.023.
Values may be sent and summed in bfloat16 or wider, within the bound.
No kernel may reach another device: no remote copies, remote signals or barrier semaphores. Data moves between devices by JAX's collectives and lax.ppermute only.
A program may use at most 64 MiB of HBM per device.

```python
import math
import jax
import jax.numpy as jnp
from jax import lax

N = 384
LAYERS = 1
TICKS = 3
CLASSES = 8
BLOCK = 32
FREQS = 16
SECTIONS = 16
DEPTH_LAYERS = 16


def touch_ends(array, own_key, smallest, high):
    longest = array.shape.index(max(array.shape))
    spots = []
    for shift in (0, 1):
        where = [jax.random.randint(jax.random.fold_in(own_key, axis), (), 0, length) for axis, length in enumerate(array.shape)]
        where[longest] = (where[longest] + shift) % array.shape[longest]
        spots.append(tuple(where))
    return array.at[spots[0]].set(smallest).at[spots[1]].set(high)


def shard_levels(own_key, dims, cuts, low, largest):
    def one(dim, parts):
        steps = jax.random.uniform(jax.random.fold_in(jax.random.fold_in(own_key, 6), dim), (parts,), jnp.float32, low / len(cuts), largest / len(cuts))
        return jnp.repeat(jnp.exp(steps), dims[dim] // parts).reshape((-1,) + (1,) * (len(dims) - dim - 1))

    gain = one(*cuts[0])
    for cut in cuts[1:]:
        gain = gain * one(*cut)
    return gain


def bell_draw(own_key, shape, scale, limit, cuts=(), held_as=jnp.bfloat16):
    gain = shard_levels(own_key, shape, cuts, -0.22, 0.18) if cuts else 1.0
    drawn = jax.random.normal(own_key, shape, jnp.float32) * scale * gain
    return jnp.minimum(jnp.maximum(drawn, -limit), limit).astype(held_as)


def setup_inputs(seed: int = 0) -> dict:
    arg_keys = jax.random.split(jax.random.key(seed), 8)
    fields_top = bell_draw(arg_keys[0], (SECTIONS, 2, FREQS, 2, N, N), 1.0, 6.0, ((0, 16), (2, 16)))
    surface = bell_draw(arg_keys[1], (TICKS - 1, 2, FREQS, 2, N, N), 1.0, 6.0, ((2, 16),))
    up_state = bell_draw(arg_keys[2], (SECTIONS, FREQS, 2, N, N), 1.0, 6.0, ((0, 16), (1, 16)))
    angular_freq = jnp.clip(0.5 + 2.0 * jax.random.uniform(arg_keys[3], (FREQS,), jnp.float32) ** shard_levels(arg_keys[3], (FREQS,), ((0, 16),), -0.2, 0.2), 0.5, 2.5)
    class_slowness = jnp.clip(jnp.exp(jax.random.uniform(arg_keys[4], (CLASSES,), jnp.float32, math.log(0.6), math.log(1.3))), 0.6, 1.3)
    velocity_class = touch_ends(jax.random.randint(arg_keys[5], (DEPTH_LAYERS, N // BLOCK, N // BLOCK), 0, CLASSES), jax.random.fold_in(arg_keys[5], 1), 0, CLASSES - 1).astype(jnp.int32)
    slowness_detail = jnp.clip(1.0 + 0.1 * jax.random.normal(arg_keys[6], (DEPTH_LAYERS, N, N), jnp.float32), 0.5, 1.5)
    return {"fields_top": fields_top, "surface": surface, "up_state": up_state, "angular_freq": angular_freq, "class_slowness": class_slowness, "velocity_class": velocity_class, "slowness_detail": slowness_detail}


DEPTH_STEP = 1.0
EPSILON = 1e-06

def make_tables(lateral):
    positions = jnp.arange(lateral, dtype=jnp.int32)
    wrapped = positions[:, None] * positions[None, :] % lateral
    angles = wrapped.astype(jnp.float32) * (2.0 * jnp.pi / lateral)
    cosine_table = jnp.cos(angles).astype(jnp.bfloat16)
    sine_table = jnp.sin(angles).astype(jnp.bfloat16)
    folded = jnp.where(positions < lateral // 2, positions, positions - lateral)
    kappa = folded.astype(jnp.float32) * (2.0 * jnp.pi / lateral)
    wavenumber_sq = kappa[:, None] ** 2 + kappa[None, :] ** 2
    return (cosine_table, sine_table, wavenumber_sq)

def cell_slowness(velocity_class, class_slowness, slowness_detail):
    count, lateral = (slowness_detail.shape[0], slowness_detail.shape[1])
    blocks = lateral // BLOCK
    onehot = (velocity_class[..., None] == jnp.arange(CLASSES, dtype=jnp.int32)).astype(jnp.float32)
    block_slow = lax.optimization_barrier(jnp.sum(onehot * class_slowness, axis=-1))
    spread = jnp.broadcast_to(block_slow[:, :, None, :, None], (count, blocks, BLOCK, blocks, BLOCK))
    slowness = spread.reshape(count, lateral, lateral) * slowness_detail
    return (slowness, lax.optimization_barrier(jnp.mean(slowness, axis=(1, 2))))

def propagate(real_part, imag_part, angular, slowness, reference_slow, cosine_table, sine_table, wavenumber_sq):
    lateral = real_part.shape[0]
    joined_cols = jnp.concatenate([cosine_table, sine_table], axis=1)
    joined_rows = jnp.concatenate([cosine_table, sine_table], axis=0)
    product = jnp.dot(jnp.concatenate([real_part, imag_part], axis=0), joined_cols, preferred_element_type=jnp.float32)
    real_cos, real_sin = (product[:lateral, :lateral], product[:lateral, lateral:])
    imag_cos, imag_sin = (product[lateral:, :lateral], product[lateral:, lateral:])
    half_real = (real_cos + imag_sin).astype(jnp.bfloat16)
    half_imag = (imag_cos - real_sin).astype(jnp.bfloat16)
    product = jnp.dot(joined_rows, jnp.concatenate([half_real, half_imag], axis=1), preferred_element_type=jnp.float32)
    cos_real, cos_imag = (product[:lateral, :lateral], product[:lateral, lateral:])
    sin_real, sin_imag = (product[lateral:, :lateral], product[lateral:, lateral:])
    spec_real = cos_real + sin_imag
    spec_imag = cos_imag - sin_real
    vertical = (angular * reference_slow) ** 2 - wavenumber_sq
    travel = jnp.sqrt(jnp.maximum(vertical, 0.0)) * DEPTH_STEP
    decay = jnp.exp(-jnp.sqrt(jnp.maximum(-vertical, 0.0)) * DEPTH_STEP) / (lateral * lateral)
    phase_real = decay * jnp.cos(travel)
    phase_imag = decay * jnp.sin(travel)
    shifted_real = (spec_real * phase_real - spec_imag * phase_imag).astype(jnp.bfloat16)
    shifted_imag = (spec_real * phase_imag + spec_imag * phase_real).astype(jnp.bfloat16)
    product = jnp.dot(joined_rows, jnp.concatenate([shifted_real, shifted_imag], axis=1), preferred_element_type=jnp.float32)
    cos_real, cos_imag = (product[:lateral, :lateral], product[:lateral, lateral:])
    sin_real, sin_imag = (product[lateral:, :lateral], product[lateral:, lateral:])
    back_real = (cos_real - sin_imag).astype(jnp.bfloat16)
    back_imag = (cos_imag + sin_real).astype(jnp.bfloat16)
    product = jnp.dot(jnp.concatenate([back_real, back_imag], axis=0), joined_cols, preferred_element_type=jnp.float32)
    real_cos, real_sin = (product[:lateral, :lateral], product[:lateral, lateral:])
    imag_cos, imag_sin = (product[lateral:, :lateral], product[lateral:, lateral:])
    space_real = real_cos - imag_sin
    space_imag = imag_cos + real_sin
    lens = angular * DEPTH_STEP * (slowness - reference_slow)
    lens_cos, lens_sin = (jnp.cos(lens), jnp.sin(lens))
    new_real = (space_real * lens_cos - space_imag * lens_sin).astype(jnp.bfloat16)
    new_imag = (space_real * lens_sin + space_imag * lens_cos).astype(jnp.bfloat16)
    return (new_real, new_imag)

def advance(fields, angular, slowness, reference_slow, tables):
    cosine_table, sine_table, wavenumber_sq = tables

    def single(real_part, imag_part, frequency):
        return propagate(real_part, imag_part, frequency, slowness, reference_slow, cosine_table, sine_table, wavenumber_sq)
    new_real, new_imag = jax.vmap(single)(fields[:, 0], fields[:, 1], angular)
    return jnp.stack([new_real, new_imag], axis=1)

def advance_pair(fields, angular, slowness, reference_slow, tables):

    def one_field(member):
        return advance(member, angular, slowness, reference_slow, tables)
    return jax.vmap(one_field)(fields)

def image_terms(fields):
    source = fields[0].astype(jnp.float32)
    receiver = fields[1].astype(jnp.float32)
    image_part = lax.optimization_barrier(jnp.sum(source[:, 0] * receiver[:, 0] + source[:, 1] * receiver[:, 1], axis=0))
    illum_part = lax.optimization_barrier(jnp.sum(source[:, 0] * source[:, 0] + source[:, 1] * source[:, 1], axis=0))
    return (image_part, illum_part)

def reference(fields_top, surface, up_state, angular_freq, class_slowness, velocity_class, slowness_detail):
    lateral = fields_top.shape[-1]
    sections = fields_top.shape[0]
    tables = make_tables(lateral)
    slowness, reference_slow = cell_slowness(velocity_class, class_slowness, slowness_detail)
    total_layers = slowness.shape[0]
    image_sum = [jnp.zeros((lateral, lateral), jnp.float32) for layer_index in range(total_layers)]
    illumination = [jnp.zeros((lateral, lateral), jnp.float32) for layer_index in range(total_layers)]
    sources = [None] * total_layers
    current = [fields_top[section] for section in range(sections)]
    for turn_index in range(TICKS):
        ended = []
        for section in range(sections):
            fields = current[section]
            for inner in range(LAYERS):
                layer_index = section * LAYERS + inner
                fields = advance_pair(fields, angular_freq, slowness[layer_index], reference_slow[layer_index], tables)
                image_part, illum_part = image_terms(fields)
                image_sum[layer_index] = image_sum[layer_index] + image_part
                illumination[layer_index] = illumination[layer_index] + illum_part
                if turn_index == TICKS - 1:
                    sources[layer_index] = fields[0]
            ended.append(fields)
        if turn_index + 1 < TICKS:
            current = [surface[turn_index]] + ended[:-1]
    image_all = jnp.stack(image_sum)
    illum_all = jnp.stack(illumination)
    damping = lax.optimization_barrier(jnp.mean(illum_all, axis=(1, 2)))
    balanced = image_all / (illum_all + damping[:, None, None])
    mean_square = lax.optimization_barrier(jnp.mean(balanced * balanced, axis=(1, 2)))
    reflect = (balanced * lax.rsqrt(mean_square + EPSILON)[:, None, None]).astype(jnp.bfloat16)
    rising_all = []
    for section in range(sections):
        if section + 1 < sections:
            rising_wave = up_state[section + 1]
        else:
            rising_wave = jnp.zeros_like(up_state[0])
        for inner in reversed(range(LAYERS)):
            layer_index = section * LAYERS + inner
            scattered = reflect[layer_index].astype(jnp.float32)[None, None] * sources[layer_index].astype(jnp.float32)
            rising_wave = (rising_wave.astype(jnp.float32) + scattered).astype(jnp.bfloat16)
            rising_wave = advance(rising_wave, angular_freq, slowness[layer_index], reference_slow[layer_index], tables)
        rising_all.append(rising_wave)
    return (reflect, jnp.stack(rising_all))
```

```python
from functools import partial

import jax
import jax.numpy as jnp
import ml_dtypes
import numpy as np
from jax import lax
from jax.experimental import pallas as pl
from jax.experimental.pallas import tpu as pltpu
from jax.sharding import PartitionSpec as P

TICKS = 3
BLOCK = 32
DEPTH_STEP = 1.0
EPSILON = 1e-06
F32 = jnp.float32
BF16 = jnp.bfloat16


def transform_tables(lateral):
    half = lateral // 2
    place = np.arange(lateral)
    wave = np.where(place <= half, place, place - half)
    angles = (place[:, None] * wave[None, :] % lateral) * (2.0 * np.pi / lateral)
    basis = np.where(place[None, :] <= half, np.cos(angles), np.sin(angles))
    basis = basis.astype(np.float32).astype(ml_dtypes.bfloat16)
    return basis, np.ascontiguousarray(basis.T)


def sincos(x):
    turns = jnp.round(x * (2.0 / np.pi))
    r = x - turns * 1.5703125
    r = r - turns * 4.837512969970703125e-4
    r = r - turns * 7.54978995489188216e-8
    z = r * r
    sin_r = r + r * z * (-1.6666654611e-1 + z * (8.3321608736e-3 + z * -1.9515295891e-4))
    cos_r = 1.0 - 0.5 * z + z * z * (4.166664568298827e-2 + z * (-1.388731625493765e-3 + z * 2.443315711809948e-5))
    quarter = turns.astype(jnp.int32)
    swap = (quarter & 1) == 1
    sin_x = jnp.where(swap, cos_r, sin_r)
    cos_x = jnp.where(swap, sin_r, cos_r)
    sin_x = jnp.where((quarter & 2) == 2, -sin_x, sin_x)
    cos_x = jnp.where(((quarter + 1) & 2) == 2, -cos_x, cos_x)
    return sin_x, cos_x


def phases_body(spot, classes, class_slow, angular, detail, phase_re, phase_im, lens_re, lens_im):
    lateral = detail.shape[0]
    blocks = lateral // BLOCK
    w = angular[0]
    lane_block = lax.broadcasted_iota(jnp.int32, (1, lateral), 1) // BLOCK
    total = jnp.zeros((8, lateral), F32)
    for i in range(blocks):
        line = jnp.zeros((1, lateral), F32)
        for j in range(blocks):
            line = jnp.where(lane_block == j, class_slow[classes[i, j]], line)
        cells = line * detail[i * BLOCK : (i + 1) * BLOCK, :]
        lens_re[i * BLOCK : (i + 1) * BLOCK, :] = cells
        total = total + cells.reshape(BLOCK // 8, 8, lateral).sum(axis=0)
    mean = jnp.sum(total) / (lateral * lateral)
    square = (w * mean) * (w * mean)
    half = lateral // 2
    step = 2.0 * np.pi / lateral

    def axis_terms(shape, dim):
        place = lax.broadcasted_iota(jnp.int32, shape, dim)
        wave = jnp.where(place <= half, place, place - half)
        kappa = wave.astype(F32) * step
        weight = jnp.where((wave == 0) | (wave == half), 1.0, 2.0)
        return kappa * kappa, weight

    lane_sq, lane_weight = axis_terms((1, lateral), 1)
    rows = 32

    def chunk(index, carry):
        here = pl.ds(pl.multiple_of(index * rows, rows), rows)
        lens_sin, lens_cos = sincos(w * DEPTH_STEP * (lens_re[here, :] - mean))
        lens_re[here, :] = lens_cos
        lens_im[here, :] = lens_sin
        place = lax.broadcasted_iota(jnp.int32, (rows, 1), 0) + index * rows
        wave = jnp.where(place <= half, place, place - half)
        kappa = wave.astype(F32) * step
        weight = jnp.where((wave == 0) | (wave == half), 1.0, 2.0)
        vertical = square - (kappa * kappa + lane_sq)
        root = jnp.sqrt(jnp.abs(vertical)) * DEPTH_STEP
        decay = jnp.where(vertical < 0.0, jnp.exp(-root), 1.0)
        decay = decay * (weight * lane_weight / (lateral * lateral))
        travel_sin, travel_cos = sincos(jnp.where(vertical > 0.0, root, 0.0))
        phase_re[here, :] = decay * travel_cos
        phase_im[here, :] = decay * travel_sin
        return carry

    lax.fori_loop(0, lateral // rows, chunk, 0, unroll=2)


def step_core(start, basis, basis_t, phase_re, phase_im, lens_re, lens_im, wide, tall, write):
    n = basis.shape[0]
    first = jnp.dot(start, basis[...], preferred_element_type=F32).astype(BF16)
    wide[:, :n] = first[:n]
    wide[:, n:] = first[n:]
    spectrum = jnp.dot(basis_t[...], wide[...], preferred_element_type=F32)
    spec_re, spec_im = spectrum[:, :n], spectrum[:, n:]
    wide[:, :n] = (spec_re * phase_re[...] - spec_im * phase_im[...]).astype(BF16)
    wide[:, n:] = (spec_re * phase_im[...] + spec_im * phase_re[...]).astype(BF16)
    back = jnp.dot(basis[...], wide[...], preferred_element_type=F32).astype(BF16)
    tall[:n, :] = back[:, :n]
    tall[n:, :] = back[:, n:]
    space = jnp.dot(tall[...], basis_t[...], preferred_element_type=F32)
    space_re, space_im = space[:n], space[n:]
    write(
        (space_re * lens_re[...] - space_im * lens_im[...]).astype(BF16),
        (space_re * lens_im[...] + space_im * lens_re[...]).astype(BF16),
    )


def entering(spot, arrived, surface, tick, kind):
    n = arrived.shape[-1]
    picked = jnp.where(spot[0] == 0, surface[tick - 1, kind, 0], arrived[...])
    return picked.reshape(2 * n, n)


def put(out):
    def write(real, imag):
        out[0] = real
        out[1] = imag

    return write


TABLES = 6


def first_body(start, *refs):
    tables, (out, wide, tall) = refs[:TABLES], refs[TABLES:]
    n = start.shape[-1]
    step_core(start[0, 0, 0].reshape(2 * n, n), *tables, wide, tall, put(out))


def later_body(tick, spot, arrived, surface, *refs):
    tables, (out, wide, tall) = refs[:TABLES], refs[TABLES:]
    step_core(entering(spot, arrived, surface, tick, 0), *tables, wide, tall, put(out))


def add_terms(source, receiver, image, illum):
    s_re, s_im = source[0].astype(F32), source[1].astype(F32)
    r_re, r_im = receiver[0].astype(F32), receiver[1].astype(F32)
    return image + (s_re * r_re + s_im * r_im), illum + (s_re * s_re + s_im * s_im)


def pieces(value):
    high = value.astype(BF16).astype(F32)
    middle = (value - high).astype(BF16).astype(F32)
    low = value - high - middle
    row = lax.broadcasted_iota(jnp.int32, (8, 128), 0)
    return jnp.where(row == 0, high, jnp.where(row == 1, middle, jnp.where(row == 2, low, 0.0)))


def first_image_body(start, source, *refs):
    tables, (out, image, illum, wide, tall) = refs[:TABLES], refs[TABLES:]
    n = start.shape[-1]
    step_core(start[0, 1, 0].reshape(2 * n, n), *tables, wide, tall, put(out))
    image[...], illum[...] = add_terms(source, out, 0.0, 0.0)


def later_image_body(tick, spot, arrived, surface, source, image_in, illum_in, *refs):
    tables, (out, image, illum, wide, tall) = refs[:TABLES], refs[TABLES:]
    step_core(entering(spot, arrived, surface, tick, 1), *tables, wide, tall, put(out))
    image[...], illum[...] = add_terms(source, out, image_in[...], illum_in[...])


def last_image_body(tick, spot, arrived, surface, source, image_in, illum_in, *refs):
    tables, (parcel, wide, tall, out) = refs[:TABLES], refs[TABLES:]
    step_core(entering(spot, arrived, surface, tick, 1), *tables, wide, tall, put(out))
    image, illum = add_terms(source, out, image_in[...], illum_in[...])
    peers, n = parcel.shape[0], parcel.shape[2]
    rows = n // peers
    parcel[:, 0:rows, :] = image.astype(BF16).reshape(peers, rows, n)
    parcel[:, rows : 2 * rows, :] = illum.astype(BF16).reshape(peers, rows, n)
    extra = pieces(jnp.sum(illum)).astype(BF16)
    for peer in range(peers):
        for lane in range(0, n, 128):
            parcel[peer, 2 * rows : 2 * rows + 8, lane : lane + 128] = extra


def balance_body(parcel, out):
    peers, height, n = parcel.shape
    rows = (height - 8) // 2
    sums = parcel[0].astype(F32)
    for peer in range(1, peers):
        sums = sums + parcel[peer].astype(F32)
    image, illum = sums[:rows], sums[rows : 2 * rows]
    damping = jnp.sum(sums[2 * rows : 2 * rows + 8, 0:1]) / (n * n)
    balanced = image / (illum + damping)
    extra = pieces(jnp.sum(balanced * balanced)).astype(BF16)
    small = balanced.astype(BF16)
    for peer in range(peers):
        out[peer, 0:rows, :] = small
        for lane in range(0, n, 128):
            out[peer, rows : rows + 8, lane : lane + 128] = extra


def upward_body(spot, parcel, rising, source, *refs):
    tables, (part, out, wide, tall) = refs[:TABLES], refs[TABLES:]
    peers, height, n = parcel.shape
    rows = height - 8
    square = jnp.zeros((8, 128), F32)
    for peer in range(peers):
        square = square + parcel[peer, rows : rows + 8, 0:128].astype(F32)
    scale = lax.rsqrt(jnp.sum(square[:, 0:1]) / (n * n) + EPSILON)
    own = parcel[pl.ds(spot[1], 1)][0, 0:rows, :]
    part[...] = (own.astype(F32) * scale).astype(BF16)
    for peer in range(peers):
        here = slice(peer * rows, (peer + 1) * rows)
        reflect = (parcel[peer, 0:rows, :].astype(F32) * scale).astype(BF16).astype(F32)
        for half in range(2):
            lifted = rising[half, here, :].astype(F32) + reflect * source[half, here, :].astype(F32)
            tall[half * n + peer * rows : half * n + (peer + 1) * rows, :] = lifted.astype(BF16)
    step_core(tall[...], *tables, wide, tall, put(out))


def passed_along(block, axis, distance):
    devices = range(lax.axis_size(axis))
    route = [(i - distance, i) for i in devices if i - distance in devices]
    return lax.ppermute(block, axis, route)


def exchanged(parcel):
    return lax.all_to_all(parcel, "freq", split_axis=0, concat_axis=0, tiled=True)


def per_device(
    fields_top, surface, up_state, angular_freq, class_slowness, velocity_class, slowness_detail
):
    n = fields_top.shape[-1]
    peers = lax.axis_size("freq")
    vmem = pl.BlockSpec(memory_space=pltpu.VMEM)
    smem = pl.BlockSpec(memory_space=pltpu.SMEM)
    field = jax.ShapeDtypeStruct((2, n, n), BF16)
    cells = jax.ShapeDtypeStruct((n, n), F32)
    work = [pltpu.VMEM((n, 2 * n), BF16), pltpu.VMEM((2 * n, n), BF16)]
    cost = pl.CostEstimate(flops=2 * 4 * 2 * n**3, transcendentals=0, bytes_accessed=8 * n * n)

    def call(body, in_specs, out_shape, scratch, name):
        return pl.pallas_call(
            body,
            in_specs=in_specs,
            out_specs=jax.tree.map(lambda _: vmem, out_shape),
            out_shape=out_shape,
            scratch_shapes=scratch,
            cost_estimate=cost,
            compiler_params=pltpu.CompilerParams(vmem_limit_bytes=14 << 20),
            name=name,
        )

    spot = jnp.stack([lax.axis_index("depth"), lax.axis_index("freq")]).astype(jnp.int32)
    basis, basis_t = (jnp.asarray(table) for table in transform_tables(n))
    phases = call(phases_body, [smem, smem, smem, smem, vmem], [cells] * 4, [], "phases")(
        spot, velocity_class[0], class_slowness, angular_freq, slowness_detail[0]
    )
    tables = (basis, basis_t, *phases)

    source = call(first_body, [vmem] * (1 + TABLES), field, work, "source_0")(
        fields_top, *tables
    )
    sent_source = passed_along(source, "depth", 1)
    receiver, image, illum = call(
        first_image_body, [vmem] * (2 + TABLES), [field, cells, cells], work, "receiver_0"
    )(fields_top, source, *tables)
    rising = passed_along(up_state[0, 0], "depth", -1)
    for tick in range(1, TICKS):
        sent_receiver = passed_along(receiver, "depth", 1)
        source = call(
            partial(later_body, tick), [smem] + [vmem] * (2 + TABLES), field, work, f"source_{tick}"
        )(spot, sent_source, surface, *tables)
        args = (spot, sent_receiver, surface, source, image, illum, *tables)
        specs = [smem] + [vmem] * (5 + TABLES)
        if tick + 1 < TICKS:
            sent_source = passed_along(source, "depth", 1)
            receiver, image, illum = call(
                partial(later_image_body, tick), specs, [field, cells, cells], work, f"receiver_{tick}"
            )(*args)
        else:
            parcel = jax.ShapeDtypeStruct((peers, 2 * (n // peers) + 8, n), BF16)
            parcel = call(
                partial(last_image_body, tick), specs, parcel, work + [pltpu.VMEM((2, n, n), BF16)], "receiver_last"
            )(*args)
    rows = n // peers
    balanced = jax.ShapeDtypeStruct((peers, rows + 8, n), BF16)
    balanced = call(balance_body, [vmem], balanced, [], "balance")(exchanged(parcel))
    part, risen = call(
        upward_body,
        [smem] + [vmem] * (3 + TABLES),
        [jax.ShapeDtypeStruct((rows, n), BF16), field],
        work,
        "upward",
    )(spot, exchanged(balanced), rising, source, *tables)
    return (part[None], risen[None, None])


def solution(mesh):
    return jax.shard_map(
        per_device,
        mesh=mesh,
        in_specs=(
            P("depth", None, "freq", None, None, None),
            P(None, None, "freq", None, None, None),
            P("depth", "freq", None, None, None),
            P("freq"),
            P(),
            P("depth", None, None),
            P("depth", None, None),
        ),
        out_specs=(P("depth", "freq", None), P("depth", "freq", None, None, None)),
        check_vma=False,
    )
```

```python
from functools import partial

import jax
import jax.numpy as jnp
import ml_dtypes
import numpy as np
from jax import lax
from jax.experimental import pallas as pl
from jax.experimental.pallas import tpu as pltpu
from jax.sharding import PartitionSpec as P

TICKS = 3
BLOCK = 32
DEPTH_STEP = 1.0
EPSILON = 1e-06
F32 = jnp.float32
BF16 = jnp.bfloat16


def transform_tables(lateral):
    half = lateral // 2
    place = np.arange(lateral)
    wave = np.where(place <= half, place, place - half)
    angles = (place[:, None] * wave[None, :] % lateral) * (2.0 * np.pi / lateral)
    basis = np.where(place[None, :] <= half, np.cos(angles), np.sin(angles))
    basis = basis.astype(np.float32).astype(ml_dtypes.bfloat16)
    return basis, np.ascontiguousarray(basis.T)


def sincos(x):
    turns = jnp.round(x * (2.0 / np.pi))
    r = x - turns * 1.5703125
    r = r - turns * 4.837512969970703125e-4
    r = r - turns * 7.54978995489188216e-8
    z = r * r
    sin_r = r + r * z * (-1.6666654611e-1 + z * (8.3321608736e-3 + z * -1.9515295891e-4))
    cos_r = 1.0 - 0.5 * z + z * z * (4.166664568298827e-2 + z * (-1.388731625493765e-3 + z * 2.443315711809948e-5))
    quarter = turns.astype(jnp.int32)
    swap = (quarter & 1) == 1
    sin_x = jnp.where(swap, cos_r, sin_r)
    cos_x = jnp.where(swap, sin_r, cos_r)
    sin_x = jnp.where((quarter & 2) == 2, -sin_x, sin_x)
    cos_x = jnp.where(((quarter + 1) & 2) == 2, -cos_x, cos_x)
    return sin_x, cos_x


def phases_body(classes, scalars, detail, phase_re, phase_im, lens_re, lens_im, kinds_of):
    lateral = detail.shape[0]
    blocks = lateral // BLOCK
    half = lateral // 2
    step = 2.0 * np.pi / lateral
    lane_block = lax.broadcasted_iota(jnp.int32, (1, lateral), 1) // BLOCK

    def axis_terms(shape, dim, offset):
        place = lax.broadcasted_iota(jnp.int32, shape, dim) + offset
        wave = jnp.where(place <= half, place, place - half)
        kappa = wave.astype(F32) * step
        weight = jnp.where((wave == 0) | (wave == half), 1.0, 2.0)
        return kappa * kappa, weight

    lane_sq, lane_weight = axis_terms((1, lateral), 1, 0)
    for i in range(blocks):
        kinds_of[i : i + 1, :] = classes[i]
    kinds = kinds_of[...]
    slow = jnp.zeros(kinds.shape, F32)
    count = scalars.shape[1] - 1
    for kind in range(count):
        slow = jnp.where(kinds == kind, scalars[0:1, kind : kind + 1], slow)
    w = scalars[0:1, count : count + 1]
    spread = jnp.zeros((blocks, lateral), F32)
    for j in range(blocks):
        spread = jnp.where(lane_block == j, slow[:, j : j + 1], spread)
    total = jnp.zeros((8, lateral), F32)
    for i in range(blocks):
        cells = spread[i : i + 1, :] * detail[i * BLOCK : (i + 1) * BLOCK, :]
        lens_re[i * BLOCK : (i + 1) * BLOCK, :] = cells
        total = total + cells.reshape(BLOCK // 8, 8, lateral).sum(axis=0)
    mean = jnp.sum(jnp.sum(total, axis=0, keepdims=True), axis=1, keepdims=True) / (lateral * lateral)
    square = (w * mean) * (w * mean)
    scale = w * DEPTH_STEP

    def phases(start, rows):
        row_sq, row_weight = axis_terms((rows, 1), 0, start)
        vertical = square - (row_sq + lane_sq)
        root = jnp.sqrt(jnp.abs(vertical)) * DEPTH_STEP
        decay = jnp.where(vertical < 0.0, jnp.exp(-root), 1.0)
        decay = decay * (row_weight * lane_weight / (lateral * lateral))
        travel_sin, travel_cos = sincos(jnp.where(vertical > 0.0, root, 0.0))
        return decay * travel_cos, decay * travel_sin

    rows = 32

    def lens(index, carry):
        here = pl.ds(pl.multiple_of(index * rows, rows), rows)
        lens_sin, lens_cos = sincos(scale * (lens_re[here, :] - mean))
        lens_re[here, :] = lens_cos
        lens_im[here, :] = lens_sin
        return carry

    lax.fori_loop(0, lateral // rows, lens, 0, unroll=2)

    def spectral(index, carry):
        start = pl.multiple_of(index * rows, rows)
        real, imag = phases(start, rows)
        for first in (0, half):
            here = pl.ds(pl.multiple_of(start + first, rows), rows)
            phase_re[here, :] = real
            phase_im[here, :] = imag
        return carry

    lax.fori_loop(0, half // rows, spectral, 0, unroll=2)
    phase_re[half : half + 8, :], phase_im[half : half + 8, :] = phases(half, 8)


def step_core(start, basis, basis_t, phase_re, phase_im, lens_re, lens_im, wide, tall, write):
    n = basis.shape[0]
    first = jnp.dot(start, basis[...], preferred_element_type=F32).astype(BF16)
    wide[:, :n] = first[:n]
    wide[:, n:] = first[n:]
    spectrum = jnp.dot(basis_t[...], wide[...], preferred_element_type=F32)
    spec_re, spec_im = spectrum[:, :n], spectrum[:, n:]
    wide[:, :n] = (spec_re * phase_re[...] - spec_im * phase_im[...]).astype(BF16)
    wide[:, n:] = (spec_re * phase_im[...] + spec_im * phase_re[...]).astype(BF16)
    back = jnp.dot(basis[...], wide[...], preferred_element_type=F32).astype(BF16)
    tall[:n, :] = back[:, :n]
    tall[n:, :] = back[:, n:]
    space = jnp.dot(tall[...], basis_t[...], preferred_element_type=F32)
    space_re, space_im = space[:n], space[n:]
    write(
        (space_re * lens_re[...] - space_im * lens_im[...]).astype(BF16),
        (space_re * lens_im[...] + space_im * lens_re[...]).astype(BF16),
    )


def entering(arrived, surface, tick, kind, tall):
    n = arrived.shape[-1]

    @pl.when(lax.axis_index("depth") == 0)
    def _():
        tall[...] = surface[tick - 1, kind, 0].reshape(2 * n, n)

    @pl.when(lax.axis_index("depth") != 0)
    def _():
        tall[...] = arrived[...].reshape(2 * n, n)

    return tall[...]


def put(out):
    def write(real, imag):
        out[0] = real
        out[1] = imag

    return write


TABLES = 6


def first_body(start, *refs):
    tables, (out, wide, tall) = refs[:TABLES], refs[TABLES:]
    n = start.shape[-1]
    step_core(start[0, 0, 0].reshape(2 * n, n), *tables, wide, tall, put(out))


def later_body(tick, arrived, surface, *refs):
    tables, (out, wide, tall) = refs[:TABLES], refs[TABLES:]
    step_core(entering(arrived, surface, tick, 0, tall), *tables, wide, tall, put(out))


def add_terms(source, receiver, image, illum):
    s_re, s_im = source[0].astype(F32), source[1].astype(F32)
    r_re, r_im = receiver[0].astype(F32), receiver[1].astype(F32)
    return image + (s_re * r_re + s_im * r_im), illum + (s_re * s_re + s_im * s_im)


def pieces(value, rows):
    high = value.astype(BF16).astype(F32)
    middle = (value - high).astype(BF16).astype(F32)
    low = value - high - middle
    row = lax.broadcasted_iota(jnp.int32, (rows, 128), 0)
    parts = jnp.where(row == 0, high, jnp.where(row == 1, middle, jnp.where(row == 2, low, 0.0)))
    return parts.astype(BF16)


def first_image_body(start, source, *refs):
    tables, (out, image, illum, wide, tall) = refs[:TABLES], refs[TABLES:]
    n = start.shape[-1]
    step_core(start[0, 1, 0].reshape(2 * n, n), *tables, wide, tall, put(out))
    image[...], illum[...] = add_terms(source, out, 0.0, 0.0)


def later_image_body(tick, arrived, surface, source, image_in, illum_in, *refs):
    tables, (out, image, illum, wide, tall) = refs[:TABLES], refs[TABLES:]
    step_core(entering(arrived, surface, tick, 1, tall), *tables, wide, tall, put(out))
    image[...], illum[...] = add_terms(source, out, image_in[...], illum_in[...])


def last_image_body(tick, rising, arrived, surface, source, image_in, illum_in, *refs):
    tables, (parcel, wide, tall, out) = refs[:TABLES], refs[TABLES:]
    peers = parcel.shape[0]
    n = illum_in.shape[0]
    rows = n // peers
    lit = 3 * rows
    total = jnp.zeros((rows, n), F32)
    for peer in range(peers):
        here = slice(peer * rows, (peer + 1) * rows)
        s_re, s_im = source[0, here, :].astype(F32), source[1, here, :].astype(F32)
        illum = illum_in[here, :] + (s_re * s_re + s_im * s_im)
        total = total + illum
        small = illum.astype(BF16)
        for lane in range(3):
            there = slice(lit + lane * rows, lit + (lane + 1) * rows)
            parcel[peer, there, :] = small[:, lane * 128 : (lane + 1) * 128]
    extra = pieces(jnp.sum(total), 16)
    for peer in range(peers):
        parcel[peer, 2 * lit : 2 * lit + 16, :] = extra
    step_core(entering(arrived, surface, tick, 1, tall), *tables, wide, tall, put(out))
    for peer in range(peers):
        here = slice(peer * rows, (peer + 1) * rows)
        image = image_in[here, :]
        for part in range(2):
            image = image + source[part, here, :].astype(F32) * out[part, here, :].astype(F32)
        small = image.astype(BF16)
        for lane in range(3):
            parcel[peer, lane * rows : (lane + 1) * rows, :] = small[:, lane * 128 : (lane + 1) * 128]


def balance_body(parcel, out):
    peers, height, lanes = parcel.shape
    lit = (height - 16) // 2
    cells = lit * lanes * peers
    sums = parcel[0].astype(F32)
    for peer in range(1, peers):
        sums = sums + parcel[peer].astype(F32)
    image, illum = sums[:lit], sums[lit : 2 * lit]
    damping = jnp.sum(sums[2 * lit :, 0:1]) / cells
    balanced = image / (illum + damping)
    small = balanced.astype(BF16)
    extra = pieces(jnp.sum(balanced * balanced), 8)
    for peer in range(peers):
        out[peer, 0:lit, :] = small
        out[peer, lit : lit + 8, :] = extra


def upward_body(parcel, rising, source, *refs):
    tables, (part, out, wide, tall) = refs[:TABLES], refs[TABLES:]
    peers, _, lanes = parcel.shape
    n = source.shape[-1]
    rows = n // peers
    square = jnp.zeros((8, lanes), F32)
    for peer in range(peers):
        square = square + parcel[peer, 3 * rows : 3 * rows + 8, :].astype(F32)
    scale = lax.rsqrt(jnp.sum(square[:, 0:1]) / (n * n) + EPSILON)
    own = (parcel[pl.ds(lax.axis_index("freq"), 1)][0].astype(F32) * scale).astype(BF16)
    for lane in range(3):
        part[:, lane * lanes : (lane + 1) * lanes] = own[lane * rows : (lane + 1) * rows]
    for peer in range(peers):
        here = slice(peer * rows, (peer + 1) * rows)
        for lane in range(3):
            there = slice(lane * lanes, (lane + 1) * lanes)
            reflect = parcel[peer, lane * rows : (lane + 1) * rows, :].astype(F32) * scale
            reflect = reflect.astype(BF16).astype(F32)
            for half in range(2):
                lifted = rising[half, here, there].astype(F32) + reflect * source[half, here, there].astype(F32)
                tall[half * n + peer * rows : half * n + (peer + 1) * rows, there] = lifted.astype(BF16)
    step_core(tall[...], *tables, wide, tall, put(out))


def passed_along(block, axis, distance):
    devices = range(lax.axis_size(axis))
    route = [(i - distance, i) for i in devices if i - distance in devices]
    return lax.ppermute(block, axis, route)


def exchanged(parcel):
    return lax.all_to_all(parcel, "freq", split_axis=0, concat_axis=0, tiled=True)


def per_device(
    fields_top, surface, up_state, angular_freq, class_slowness, velocity_class, slowness_detail
):
    n = fields_top.shape[-1]
    peers = lax.axis_size("freq")
    vmem = pl.BlockSpec(memory_space=pltpu.VMEM)
    field = jax.ShapeDtypeStruct((2, n, n), BF16)
    cells = jax.ShapeDtypeStruct((n, n), F32)
    work = [pltpu.VMEM((n, 2 * n), BF16), pltpu.VMEM((2 * n, n), BF16)]
    cost = pl.CostEstimate(flops=2 * 4 * 2 * n**3, transcendentals=0, bytes_accessed=8 * n * n)

    def call(body, in_specs, out_shape, scratch):
        return pl.pallas_call(
            body,
            in_specs=in_specs,
            out_specs=jax.tree.map(lambda _: vmem, out_shape),
            out_shape=out_shape,
            scratch_shapes=scratch,
            cost_estimate=cost,
            compiler_params=pltpu.CompilerParams(vmem_limit_bytes=14 << 20),
        )

    rows = n // peers
    lit = rows * n // 128
    basis, basis_t = (jnp.asarray(table) for table in transform_tables(n))
    scalars = jnp.concatenate([class_slowness, angular_freq])[None]
    kinds = velocity_class.transpose(1, 0, 2)
    scratch = [pltpu.VMEM((kinds.shape[0], kinds.shape[2]), jnp.int32)]
    phases = call(phases_body, [vmem] * 3, [cells] * 4, scratch)(kinds, scalars, slowness_detail[0])
    tables = (basis, basis_t, *phases)
    source = call(first_body, [vmem] * (1 + TABLES), field, work)(fields_top, *tables)
    sent_source = passed_along(source, "depth", 1)
    receiver, image, illum = call(
        first_image_body, [vmem] * (2 + TABLES), [field, cells, cells], work
    )(fields_top, source, *tables)
    rising = passed_along(up_state[0, 0], "depth", -1)
    for tick in range(1, TICKS):
        sent_receiver = passed_along(receiver, "depth", 1)
        source = call(
            partial(later_body, tick), [vmem] * (2 + TABLES), field, work
        )(sent_source, surface, *tables)
        args = (sent_receiver, surface, source, image, illum, *tables)
        specs = [vmem] * (5 + TABLES)
        if tick + 1 < TICKS:
            sent_source = passed_along(source, "depth", 1)
            receiver, image, illum = call(
                partial(later_image_body, tick), specs, [field, cells, cells], work
            )(*args)
        else:
            parcel = jax.ShapeDtypeStruct((peers, 2 * lit + 16, 128), BF16)
            parcel = call(
                partial(last_image_body, tick),
                [vmem] + specs,
                parcel,
                work + [pltpu.VMEM((2, n, n), BF16)],
            )(rising, *args)
    balanced = jax.ShapeDtypeStruct((peers, lit + 8, 128), BF16)
    balanced = call(balance_body, [vmem], balanced, [])(exchanged(parcel))
    part, risen = call(
        upward_body, [vmem] * (3 + TABLES), [jax.ShapeDtypeStruct((rows, n), BF16), field], work
    )(exchanged(balanced), rising, source, *tables)
    return (part[None], risen[None, None])


def solution(mesh):
    return jax.shard_map(
        per_device,
        mesh=mesh,
        in_specs=(
            P("depth", None, "freq", None, None, None),
            P(None, None, "freq", None, None, None),
            P("depth", "freq", None, None, None),
            P("freq"),
            P(),
            P("depth", None, None),
            P("depth", None, None),
        ),
        out_specs=(P("depth", "freq", None), P("depth", "freq", None, None, None)),
        check_vma=False,
    )
```

```python
from functools import partial

import jax
import jax.numpy as jnp
import ml_dtypes
import numpy as np
from jax import lax
from jax.experimental import pallas as pl
from jax.experimental.pallas import tpu as pltpu
from jax.sharding import PartitionSpec as P

TICKS = 3
BLOCK = 32
DEPTH_STEP = 1.0
EPSILON = 1e-06
F32 = jnp.float32
BF16 = jnp.bfloat16


def transform_tables(lateral):
    half = lateral // 2
    place = np.arange(lateral)
    wave = np.where(place <= half, place, place - half)
    angles = (place[:, None] * wave[None, :] % lateral) * (2.0 * np.pi / lateral)
    basis = np.where(place[None, :] <= half, np.cos(angles), np.sin(angles))
    basis = basis.astype(np.float32).astype(ml_dtypes.bfloat16)
    return basis, np.ascontiguousarray(basis.T)


def sincos(x):
    y = x * 0.25
    z = y * y
    s = y + y * z * (-1 / 6 + z * (1 / 120 + z * (-1 / 5040 + z * (1 / 362880 + z * (-1 / 39916800)))))
    c = 1.0 + z * (-1 / 2 + z * (1 / 24 + z * (-1 / 720 + z * (1 / 40320 + z * (-1 / 3628800 + z * (1 / 479001600))))))
    s2 = s * c
    s2 = s2 + s2
    c2 = 1.0 - 2.0 * (s * s)
    s4 = s2 * c2
    return s4 + s4, 1.0 - 2.0 * (s2 * s2)


def opening_body(angular, fields, basis_hbm, basis_t_hbm, classes_hbm, slow_hbm, detail_hbm,
                 basis, basis_t, phase_re, phase_im, lens_re, lens_im, receiver, out,
                 classes, class_slow, detail, kinds_of, wide, tall, spectrum, start, sems):
    pairs = (
        (fields.at[0, 0, 0], start),
        (basis_hbm, basis),
        (basis_t_hbm, basis_t),
        (classes_hbm, classes),
        (slow_hbm, class_slow),
        (detail_hbm, detail),
        (fields.at[0, 1, 0], receiver),
    )
    copies = [pltpu.make_async_copy(a, b, sems.at[k]) for k, (a, b) in enumerate(pairs)]
    for copy in copies:
        copy.start()
    for copy in copies[:3]:
        copy.wait()
    spectrum[...] = to_spectrum(start[...].reshape(tall.shape), basis, basis_t, wide)
    lateral = detail.shape[0]
    blocks = lateral // BLOCK
    half = lateral // 2
    step = 2.0 * np.pi / lateral
    lane_block = lax.broadcasted_iota(jnp.int32, (1, lateral), 1) // BLOCK

    def axis_terms(shape, dim, offset):
        place = lax.broadcasted_iota(jnp.int32, shape, dim) + offset
        wave = jnp.where(place <= half, place, place - half)
        kappa = wave.astype(F32) * step
        weight = jnp.where((wave == 0) | (wave == half), 1.0, 2.0)
        return kappa * kappa, weight

    lane_sq, lane_weight = axis_terms((1, lateral), 1, 0)
    for copy in copies[3:5]:
        copy.wait()
    for i in range(blocks):
        kinds_of[i : i + 1, :] = classes[i]
    kinds = kinds_of[...]
    slow = jnp.zeros(kinds.shape, F32)
    for kind in range(class_slow.shape[1]):
        slow = jnp.where(kinds == kind, class_slow[0:1, kind : kind + 1], slow)
    w = angular[0]
    spread = jnp.zeros((blocks, lateral), F32)
    for j in range(blocks):
        spread = jnp.where(lane_block == j, slow[:, j : j + 1], spread)
    copies[5].wait()
    total = jnp.zeros((8, lateral), F32)
    for i in range(blocks):
        cells = spread[i : i + 1, :] * detail[i * BLOCK : (i + 1) * BLOCK, :]
        lens_re[i * BLOCK : (i + 1) * BLOCK, :] = cells
        total = total + cells.reshape(BLOCK // 8, 8, lateral).sum(axis=0)
    mean = jnp.sum(jnp.sum(total, axis=0, keepdims=True), axis=1, keepdims=True) / (lateral * lateral)
    square = (w * mean) * (w * mean)
    scale = w * DEPTH_STEP

    def phases(start, rows):
        row_sq, row_weight = axis_terms((rows, 1), 0, start)
        vertical = square - (row_sq + lane_sq)
        root = jnp.sqrt(jnp.abs(vertical)) * DEPTH_STEP
        decay = jnp.where(vertical < 0.0, jnp.exp(-root), 1.0)
        decay = decay * (row_weight * lane_weight / (lateral * lateral))
        travel_sin, travel_cos = sincos(jnp.where(vertical > 0.0, root, 0.0))
        return decay * travel_cos, decay * travel_sin

    rows = 32

    def lens(index, carry):
        here = pl.ds(pl.multiple_of(index * rows, rows), rows)
        lens_sin, lens_cos = sincos(scale * (lens_re[here, :] - mean))
        lens_re[here, :] = lens_cos
        lens_im[here, :] = lens_sin
        return carry

    lax.fori_loop(0, lateral // rows, lens, 0, unroll=2)

    def spectral(index, carry):
        start = pl.multiple_of(index * rows, rows)
        real, imag = phases(start, rows)
        for first in (0, half):
            here = pl.ds(pl.multiple_of(start + first, rows), rows)
            phase_re[here, :] = real
            phase_im[here, :] = imag
        return carry

    lax.fori_loop(0, half // rows, spectral, 0, unroll=2)
    phase_re[half : half + 8, :], phase_im[half : half + 8, :] = phases(half, 8)
    from_spectrum(
        spectrum[...], basis, basis_t, phase_re, phase_im, lens_re, lens_im, wide, tall, put(out)
    )
    copies[6].wait()


def step_core(start, basis, basis_t, phase_re, phase_im, lens_re, lens_im, wide, tall, write):
    spectrum = to_spectrum(start, basis, basis_t, wide)
    from_spectrum(spectrum, basis, basis_t, phase_re, phase_im, lens_re, lens_im, wide, tall, write)


def to_spectrum(start, basis, basis_t, wide):
    n = basis.shape[0]
    first = jnp.dot(start, basis[...], preferred_element_type=F32).astype(BF16)
    wide[:, :n] = first[:n]
    wide[:, n:] = first[n:]
    return jnp.dot(basis_t[...], wide[...], preferred_element_type=F32)


def from_spectrum(spectrum, basis, basis_t, phase_re, phase_im, lens_re, lens_im, wide, tall, write):
    n = basis.shape[0]
    spec_re, spec_im = spectrum[:, :n], spectrum[:, n:]
    wide[:, :n] = (spec_re * phase_re[...] - spec_im * phase_im[...]).astype(BF16)
    wide[:, n:] = (spec_re * phase_im[...] + spec_im * phase_re[...]).astype(BF16)
    back = jnp.dot(basis[...], wide[...], preferred_element_type=F32).astype(BF16)
    tall[:n, :] = back[:, :n]
    tall[n:, :] = back[:, n:]
    space = jnp.dot(tall[...], basis_t[...], preferred_element_type=F32)
    space_re, space_im = space[:n], space[n:]
    write(
        (space_re * lens_re[...] - space_im * lens_im[...]).astype(BF16),
        (space_re * lens_im[...] + space_im * lens_re[...]).astype(BF16),
    )


def entering(arrived, surface, tick, kind, tall):
    n = arrived.shape[-1]

    @pl.when(lax.axis_index("depth") == 0)
    def _():
        tall[...] = surface[tick - 1, kind, 0].reshape(2 * n, n)

    @pl.when(lax.axis_index("depth") != 0)
    def _():
        tall[...] = arrived[...].reshape(2 * n, n)

    return tall[...]


def put(out):
    def write(real, imag):
        out[0] = real
        out[1] = imag

    return write


TABLES = 6


def later_body(tick, arrived, surface, *refs):
    tables, (out, wide, tall) = refs[:TABLES], refs[TABLES:]
    step_core(entering(arrived, surface, tick, 0, tall), *tables, wide, tall, put(out))


def add_terms(source, receiver, image, illum):
    s_re, s_im = source[0].astype(F32), source[1].astype(F32)
    r_re, r_im = receiver[0].astype(F32), receiver[1].astype(F32)
    return image + (s_re * r_re + s_im * r_im), illum + (s_re * s_re + s_im * s_im)


def pieces(value, rows):
    high = value.astype(BF16).astype(F32)
    middle = (value - high).astype(BF16).astype(F32)
    low = value - high - middle
    row = lax.broadcasted_iota(jnp.int32, (rows, 128), 0)
    parts = jnp.where(row == 0, high, jnp.where(row == 1, middle, jnp.where(row == 2, low, 0.0)))
    return parts.astype(BF16)


def first_image_body(start, source, *refs):
    tables, (out, image, illum, wide, tall) = refs[:TABLES], refs[TABLES:]
    n = start.shape[-1]
    step_core(start[...].reshape(2 * n, n), *tables, wide, tall, put(out))
    image[...], illum[...] = add_terms(source, out, 0.0, 0.0)


def later_image_body(tick, arrived, surface, source, image_in, illum_in, *refs):
    tables, (out, image, illum, wide, tall) = refs[:TABLES], refs[TABLES:]
    step_core(entering(arrived, surface, tick, 1, tall), *tables, wide, tall, put(out))
    image[...], illum[...] = add_terms(source, out, image_in[...], illum_in[...])


def last_image_body(tick, rising, arrived, surface, source, image_in, illum_in, *refs):
    tables, (parcel, wide, tall, out) = refs[:TABLES], refs[TABLES:]
    peers = parcel.shape[0]
    n = illum_in.shape[0]
    rows = n // peers
    lit = 3 * rows
    total = jnp.zeros((rows, n), F32)
    for peer in range(peers):
        here = slice(peer * rows, (peer + 1) * rows)
        s_re, s_im = source[0, here, :].astype(F32), source[1, here, :].astype(F32)
        illum = illum_in[here, :] + (s_re * s_re + s_im * s_im)
        total = total + illum
        small = illum.astype(BF16)
        for lane in range(3):
            there = slice(lit + lane * rows, lit + (lane + 1) * rows)
            parcel[peer, there, :] = small[:, lane * 128 : (lane + 1) * 128]
    extra = pieces(jnp.sum(total), 16)
    for peer in range(peers):
        parcel[peer, 2 * lit : 2 * lit + 16, :] = extra
    step_core(entering(arrived, surface, tick, 1, tall), *tables, wide, tall, put(out))
    for peer in range(peers):
        here = slice(peer * rows, (peer + 1) * rows)
        image = image_in[here, :]
        for part in range(2):
            image = image + source[part, here, :].astype(F32) * out[part, here, :].astype(F32)
        small = image.astype(BF16)
        for lane in range(3):
            parcel[peer, lane * rows : (lane + 1) * rows, :] = small[:, lane * 128 : (lane + 1) * 128]


def balance_body(parcel, out):
    peers, height, lanes = parcel.shape
    lit = (height - 16) // 2
    cells = lit * lanes * peers
    sums = parcel[0].astype(F32)
    for peer in range(1, peers):
        sums = sums + parcel[peer].astype(F32)
    image, illum = sums[:lit], sums[lit : 2 * lit]
    damping = jnp.sum(sums[2 * lit :, 0:1]) / cells
    balanced = image / (illum + damping)
    small = balanced.astype(BF16)
    extra = pieces(jnp.sum(balanced * balanced), 8)
    for peer in range(peers):
        out[peer, 0:lit, :] = small
        out[peer, lit : lit + 8, :] = extra


def upward_body(parcel, rising, source, *refs):
    tables, (part, out, wide, tall) = refs[:TABLES], refs[TABLES:]
    peers, _, lanes = parcel.shape
    n = source.shape[-1]
    rows = n // peers
    square = jnp.zeros((8, lanes), F32)
    for peer in range(peers):
        square = square + parcel[peer, 3 * rows : 3 * rows + 8, :].astype(F32)
    scale = lax.rsqrt(jnp.sum(square[:, 0:1]) / (n * n) + EPSILON)
    own = (parcel[pl.ds(lax.axis_index("freq"), 1)][0].astype(F32) * scale).astype(BF16)
    for lane in range(3):
        part[:, lane * lanes : (lane + 1) * lanes] = own[lane * rows : (lane + 1) * rows]
    for peer in range(peers):
        here = slice(peer * rows, (peer + 1) * rows)
        for lane in range(3):
            there = slice(lane * lanes, (lane + 1) * lanes)
            reflect = parcel[peer, lane * rows : (lane + 1) * rows, :].astype(F32) * scale
            reflect = reflect.astype(BF16).astype(F32)
            for half in range(2):
                lifted = rising[half, here, there].astype(F32) + reflect * source[half, here, there].astype(F32)
                tall[half * n + peer * rows : half * n + (peer + 1) * rows, there] = lifted.astype(BF16)
    step_core(tall[...], *tables, wide, tall, put(out))


def passed_along(block, axis, distance):
    devices = range(lax.axis_size(axis))
    route = [(i - distance, i) for i in devices if i - distance in devices]
    return lax.ppermute(block, axis, route)


def exchanged(parcel):
    return lax.all_to_all(parcel, "freq", split_axis=0, concat_axis=0, tiled=True)


def per_device(
    fields_top, surface, up_state, angular_freq, class_slowness, velocity_class, slowness_detail
):
    n = fields_top.shape[-1]
    peers = lax.axis_size("freq")
    vmem = pl.BlockSpec(memory_space=pltpu.VMEM)
    field = jax.ShapeDtypeStruct((2, n, n), BF16)
    cells = jax.ShapeDtypeStruct((n, n), F32)
    work = [pltpu.VMEM((n, 2 * n), BF16), pltpu.VMEM((2 * n, n), BF16)]
    cost = pl.CostEstimate(flops=2 * 4 * 2 * n**3, transcendentals=0, bytes_accessed=8 * n * n)

    def call(body, in_specs, out_shape, scratch):
        return pl.pallas_call(
            body,
            in_specs=in_specs,
            out_specs=jax.tree.map(lambda _: vmem, out_shape),
            out_shape=out_shape,
            scratch_shapes=scratch,
            cost_estimate=cost,
            compiler_params=pltpu.CompilerParams(vmem_limit_bytes=14 << 20),
        )

    rows = n // peers
    lit = rows * n // 128
    basis, basis_t = (jnp.asarray(table) for table in transform_tables(n))
    small = (velocity_class.transpose(1, 0, 2), class_slowness[None], slowness_detail[0])
    whole = (fields_top, basis, basis_t, *small)
    table = jax.ShapeDtypeStruct((n, n), BF16)
    scratch = [pltpu.VMEM(a.shape, a.dtype) for a in small]
    scratch += [pltpu.VMEM((small[0].shape[0], small[0].shape[2]), jnp.int32)] + work
    scratch += [pltpu.VMEM((n, 2 * n), F32), pltpu.VMEM((2, n, n), BF16), pltpu.SemaphoreType.DMA((7,))]
    *tables, receiver_top, source = call(
        opening_body,
        [pl.BlockSpec(memory_space=pltpu.SMEM)] + [pl.BlockSpec(memory_space=pltpu.HBM)] * len(whole),
        [table] * 2 + [cells] * 4 + [field] * 2,
        scratch,
    )(angular_freq, *(pltpu.with_memory_space_constraint(a, pltpu.HBM) for a in whole))
    sent_source = passed_along(source, "depth", 1)
    receiver, image, illum = call(
        first_image_body, [vmem] * (2 + TABLES), [field, cells, cells], work
    )(receiver_top, source, *tables)
    rising = passed_along(up_state[0, 0], "depth", -1)
    for tick in range(1, TICKS):
        sent_receiver = passed_along(receiver, "depth", 1)
        source = call(partial(later_body, tick), [vmem] * (2 + TABLES), field, work)(sent_source, surface, *tables)
        args = (sent_receiver, surface, source, image, illum, *tables)
        specs = [vmem] * (5 + TABLES)
        if tick + 1 < TICKS:
            sent_source = passed_along(source, "depth", 1)
            receiver, image, illum = call(partial(later_image_body, tick), specs, [field, cells, cells], work)(*args)
        else:
            parcel = jax.ShapeDtypeStruct((peers, 2 * lit + 16, 128), BF16)
            parcel = call(
                partial(last_image_body, tick), [vmem] + specs, parcel, work + [pltpu.VMEM((2, n, n), BF16)]
            )(rising, *args)
    balanced = jax.ShapeDtypeStruct((peers, lit + 8, 128), BF16)
    balanced = call(balance_body, [vmem], balanced, [])(exchanged(parcel))
    part, risen = call(
        upward_body, [vmem] * (3 + TABLES), [jax.ShapeDtypeStruct((rows, n), BF16), field], work
    )(exchanged(balanced), rising, source, *tables)
    return (part[None], risen[None, None])


def solution(mesh):
    return jax.shard_map(
        per_device,
        mesh=mesh,
        in_specs=(
            P("depth", None, "freq", None, None, None),
            P(None, None, "freq", None, None, None),
            P("depth", "freq", None, None, None),
            P("freq"),
            P(),
            P("depth", None, None),
            P("depth", None, None),
        ),
        out_specs=(P("depth", "freq", None), P("depth", "freq", None, None, None)),
        check_vma=False,
    )
```

```python
from functools import partial

import jax
import jax.numpy as jnp
import ml_dtypes
import numpy as np
from jax import lax
from jax.experimental import pallas as pl
from jax.experimental.pallas import tpu as pltpu
from jax.sharding import PartitionSpec as P

TICKS = 3
BLOCK = 32
DEPTH_STEP = 1.0
EPSILON = 1e-06
F32 = jnp.float32
BF16 = jnp.bfloat16


def transform_tables(lateral):
    half = lateral // 2
    place = np.arange(lateral)
    wave = np.where(place <= half, place, place - half)
    angles = (place[:, None] * wave[None, :] % lateral) * (2.0 * np.pi / lateral)
    basis = np.where(place[None, :] <= half, np.cos(angles), np.sin(angles))
    basis = basis.astype(np.float32).astype(ml_dtypes.bfloat16)
    return basis, np.ascontiguousarray(basis.T)


def sincos(x):
    y = x * 0.25
    z = y * y
    s = y + y * z * (-1 / 6 + z * (1 / 120 + z * (-1 / 5040 + z * (1 / 362880 + z * (-1 / 39916800)))))
    c = 1.0 + z * (-1 / 2 + z * (1 / 24 + z * (-1 / 720 + z * (1 / 40320 + z * (-1 / 3628800 + z * (1 / 479001600))))))
    s2 = s * c
    s2 = s2 + s2
    c2 = 1.0 - 2.0 * (s * s)
    s4 = s2 * c2
    return s4 + s4, 1.0 - 2.0 * (s2 * s2)


def opening_body(angular, fields, basis_hbm, basis_t_hbm, classes_hbm, slow_hbm, detail_hbm,
                 basis, basis_t, phase_re, phase_im, lens_re, lens_im, receiver, out,
                 classes, class_slow, detail, kinds_of, wide, tall, spectrum, start, sems):
    pairs = (
        (fields.at[0, 0, 0], start),
        (basis_hbm, basis),
        (basis_t_hbm, basis_t),
        (classes_hbm, classes),
        (slow_hbm, class_slow),
        (detail_hbm, detail),
        (fields.at[0, 1, 0], receiver),
    )
    copies = [pltpu.make_async_copy(a, b, sems.at[k]) for k, (a, b) in enumerate(pairs)]
    for copy in copies:
        copy.start()
    for copy in copies[:3]:
        copy.wait()
    spectrum[...] = to_spectrum(start[...].reshape(tall.shape), basis, basis_t, wide)
    lateral = detail.shape[0]
    blocks = lateral // BLOCK
    half = lateral // 2
    step = 2.0 * np.pi / lateral
    lane_block = lax.broadcasted_iota(jnp.int32, (1, lateral), 1) // BLOCK

    def axis_terms(shape, dim, offset):
        place = lax.broadcasted_iota(jnp.int32, shape, dim) + offset
        wave = jnp.where(place <= half, place, place - half)
        kappa = wave.astype(F32) * step
        weight = jnp.where((wave == 0) | (wave == half), 1.0, 2.0)
        return kappa * kappa, weight

    lane_sq, lane_weight = axis_terms((1, lateral), 1, 0)
    for copy in copies[3:5]:
        copy.wait()
    for i in range(blocks):
        kinds_of[i : i + 1, :] = classes[i]
    kinds = kinds_of[...]
    slow = jnp.zeros(kinds.shape, F32)
    for kind in range(class_slow.shape[1]):
        slow = jnp.where(kinds == kind, class_slow[0:1, kind : kind + 1], slow)
    w = angular[0]
    spread = jnp.zeros((blocks, lateral), F32)
    for j in range(blocks):
        spread = jnp.where(lane_block == j, slow[:, j : j + 1], spread)
    copies[5].wait()
    total = jnp.zeros((8, lateral), F32)
    for i in range(blocks):
        cells = spread[i : i + 1, :] * detail[i * BLOCK : (i + 1) * BLOCK, :]
        lens_re[i * BLOCK : (i + 1) * BLOCK, :] = cells
        total = total + cells.reshape(BLOCK // 8, 8, lateral).sum(axis=0)
    mean = jnp.sum(jnp.sum(total, axis=0, keepdims=True), axis=1, keepdims=True) / (lateral * lateral)
    square = (w * mean) * (w * mean)
    scale = w * DEPTH_STEP

    def phases(start, rows):
        row_sq, row_weight = axis_terms((rows, 1), 0, start)
        vertical = square - (row_sq + lane_sq)
        root = jnp.sqrt(jnp.abs(vertical)) * DEPTH_STEP
        decay = jnp.where(vertical < 0.0, jnp.exp(-root), 1.0)
        decay = decay * (row_weight * lane_weight / (lateral * lateral))
        travel_sin, travel_cos = sincos(jnp.where(vertical > 0.0, root, 0.0))
        return decay * travel_cos, decay * travel_sin

    rows = 32

    def spectral(index, carry):
        start = pl.multiple_of(index * rows, rows)
        real, imag = phases(start, rows)
        for first in (0, half):
            here = pl.ds(pl.multiple_of(start + first, rows), rows)
            phase_re[here, :] = real
            phase_im[here, :] = imag
        return carry

    lax.fori_loop(0, half // rows, spectral, 0, unroll=2)
    phase_re[half : half + 8, :], phase_im[half : half + 8, :] = phases(half, 8)
    for first in range(0, lateral, rows):
        here = slice(first, first + rows)
        lens_sin, lens_cos = sincos(scale * (lens_re[here, :] - mean))
        lens_re[here, :] = lens_cos
        lens_im[here, :] = lens_sin
    from_spectrum(
        spectrum[...], basis, basis_t, phase_re, phase_im, lens_re, lens_im, wide, tall, put(out)
    )
    copies[6].wait()


def step_core(start, basis, basis_t, phase_re, phase_im, lens_re, lens_im, wide, tall, write):
    spectrum = to_spectrum(start, basis, basis_t, wide)
    from_spectrum(spectrum, basis, basis_t, phase_re, phase_im, lens_re, lens_im, wide, tall, write)


def to_spectrum(start, basis, basis_t, wide):
    n = basis.shape[0]
    first = jnp.dot(start, basis[...], preferred_element_type=F32).astype(BF16)
    wide[:, :n] = first[:n]
    wide[:, n:] = first[n:]
    return jnp.dot(basis_t[...], wide[...], preferred_element_type=F32)


def from_spectrum(spectrum, basis, basis_t, phase_re, phase_im, lens_re, lens_im, wide, tall, write):
    n = basis.shape[0]
    spec_re, spec_im = spectrum[:, :n], spectrum[:, n:]
    wide[:, :n] = (spec_re * phase_re[...] - spec_im * phase_im[...]).astype(BF16)
    wide[:, n:] = (spec_re * phase_im[...] + spec_im * phase_re[...]).astype(BF16)
    back = jnp.dot(basis[...], wide[...], preferred_element_type=F32).astype(BF16)
    tall[:n, :] = back[:, :n]
    tall[n:, :] = back[:, n:]
    space = jnp.dot(tall[...], basis_t[...], preferred_element_type=F32)
    space_re, space_im = space[:n], space[n:]
    write(
        (space_re * lens_re[...] - space_im * lens_im[...]).astype(BF16),
        (space_re * lens_im[...] + space_im * lens_re[...]).astype(BF16),
    )


def entering(arrived, surface, tick, kind, tall):
    n = arrived.shape[-1]

    @pl.when(lax.axis_index("depth") == 0)
    def _():
        tall[...] = surface[tick - 1, kind, 0].reshape(2 * n, n)

    @pl.when(lax.axis_index("depth") != 0)
    def _():
        tall[...] = arrived[...].reshape(2 * n, n)

    return tall[...]


def put(out):
    def write(real, imag):
        out[0] = real
        out[1] = imag

    return write


TABLES = 6


def later_body(tick, arrived, surface, *refs):
    tables, (out, wide, tall) = refs[:TABLES], refs[TABLES:]
    step_core(entering(arrived, surface, tick, 0, tall), *tables, wide, tall, put(out))


def add_terms(source, receiver, image, illum):
    s_re, s_im = source[0].astype(F32), source[1].astype(F32)
    r_re, r_im = receiver[0].astype(F32), receiver[1].astype(F32)
    return image + (s_re * r_re + s_im * r_im), illum + (s_re * s_re + s_im * s_im)


def pieces(value, rows):
    high = value.astype(BF16).astype(F32)
    middle = (value - high).astype(BF16).astype(F32)
    low = value - high - middle
    row = lax.broadcasted_iota(jnp.int32, (rows, 128), 0)
    parts = jnp.where(row == 0, high, jnp.where(row == 1, middle, jnp.where(row == 2, low, 0.0)))
    return parts.astype(BF16)


def first_image_body(start, source, *refs):
    tables, (out, image, illum, wide, tall) = refs[:TABLES], refs[TABLES:]
    n = start.shape[-1]
    step_core(start[...].reshape(2 * n, n), *tables, wide, tall, put(out))
    image[...], illum[...] = add_terms(source, out, 0.0, 0.0)


def later_image_body(tick, arrived, surface, source, image_in, illum_in, *refs):
    tables, (out, image, illum, wide, tall) = refs[:TABLES], refs[TABLES:]
    step_core(entering(arrived, surface, tick, 1, tall), *tables, wide, tall, put(out))
    image[...], illum[...] = add_terms(source, out, image_in[...], illum_in[...])


def last_source_body(tick, arrived, surface, illum_in, *refs):
    tables, (out, parcel, wide, tall) = refs[:TABLES], refs[TABLES:]
    step_core(entering(arrived, surface, tick, 0, tall), *tables, wide, tall, put(out))
    peers = parcel.shape[0]
    n = illum_in.shape[0]
    rows = n // peers
    lit = 3 * rows
    total = jnp.zeros((rows, n), F32)
    for peer in range(peers):
        here = slice(peer * rows, (peer + 1) * rows)
        s_re, s_im = out[0, here, :].astype(F32), out[1, here, :].astype(F32)
        illum = illum_in[here, :] + (s_re * s_re + s_im * s_im)
        total = total + illum
        small = illum.astype(BF16)
        for lane in range(3):
            there = slice(lit + lane * rows, lit + (lane + 1) * rows)
            parcel[peer, there, :] = small[:, lane * 128 : (lane + 1) * 128]
    extra = pieces(jnp.sum(total), 16)
    for peer in range(peers):
        parcel[peer, 2 * lit : 2 * lit + 16, :] = extra
        parcel[peer, 0:lit, :] = jnp.zeros((lit, 128), BF16)


def last_image_body(tick, begun, rising, arrived, surface, source, image_in, *refs):
    tables, (parcel, wide, tall, out) = refs[:TABLES], refs[TABLES:]
    peers = parcel.shape[0]
    n = image_in.shape[0]
    rows = n // peers
    step_core(entering(arrived, surface, tick, 1, tall), *tables, wide, tall, put(out))
    for peer in range(peers):
        here = slice(peer * rows, (peer + 1) * rows)
        image = image_in[here, :]
        for part in range(2):
            image = image + source[part, here, :].astype(F32) * out[part, here, :].astype(F32)
        small = image.astype(BF16)
        for lane in range(3):
            parcel[peer, lane * rows : (lane + 1) * rows, :] = small[:, lane * 128 : (lane + 1) * 128]


def balance_body(parcel, out):
    peers, height, lanes = parcel.shape
    lit = (height - 16) // 2
    cells = lit * lanes * peers
    sums = parcel[0].astype(F32)
    for peer in range(1, peers):
        sums = sums + parcel[peer].astype(F32)
    image, illum = sums[:lit], sums[lit : 2 * lit]
    damping = jnp.sum(sums[2 * lit :, 0:1]) / cells
    balanced = image / (illum + damping)
    small = balanced.astype(BF16)
    extra = pieces(jnp.sum(balanced * balanced), 8)
    for peer in range(peers):
        out[peer, 0:lit, :] = small
        out[peer, lit : lit + 8, :] = extra


def upward_body(parcel, rising, source, *refs):
    tables, (part, out, wide, tall) = refs[:TABLES], refs[TABLES:]
    peers, _, lanes = parcel.shape
    n = source.shape[-1]
    rows = n // peers
    square = jnp.zeros((8, lanes), F32)
    for peer in range(peers):
        square = square + parcel[peer, 3 * rows : 3 * rows + 8, :].astype(F32)
    scale = lax.rsqrt(jnp.sum(square[:, 0:1]) / (n * n) + EPSILON)
    own = (parcel[pl.ds(lax.axis_index("freq"), 1)][0].astype(F32) * scale).astype(BF16)
    for lane in range(3):
        part[:, lane * lanes : (lane + 1) * lanes] = own[lane * rows : (lane + 1) * rows]
    for peer in range(peers):
        here = slice(peer * rows, (peer + 1) * rows)
        for lane in range(3):
            there = slice(lane * lanes, (lane + 1) * lanes)
            reflect = parcel[peer, lane * rows : (lane + 1) * rows, :].astype(F32) * scale
            reflect = reflect.astype(BF16).astype(F32)
            for half in range(2):
                lifted = rising[half, here, there].astype(F32) + reflect * source[half, here, there].astype(F32)
                tall[half * n + peer * rows : half * n + (peer + 1) * rows, there] = lifted.astype(BF16)
    step_core(tall[...], *tables, wide, tall, put(out))


def passed_along(block, axis, distance):
    devices = range(lax.axis_size(axis))
    route = [(i - distance, i) for i in devices if i - distance in devices]
    return lax.ppermute(block, axis, route)


def exchanged(parcel):
    return lax.all_to_all(parcel, "freq", split_axis=0, concat_axis=0, tiled=True)


def per_device(
    fields_top, surface, up_state, angular_freq, class_slowness, velocity_class, slowness_detail
):
    n = fields_top.shape[-1]
    peers = lax.axis_size("freq")
    vmem = pl.BlockSpec(memory_space=pltpu.VMEM)
    field = jax.ShapeDtypeStruct((2, n, n), BF16)
    cells = jax.ShapeDtypeStruct((n, n), F32)
    work = [pltpu.VMEM((n, 2 * n), BF16), pltpu.VMEM((2 * n, n), BF16)]
    cost = pl.CostEstimate(flops=2 * 4 * 2 * n**3, transcendentals=0, bytes_accessed=8 * n * n)

    def call(body, in_specs, out_shape, scratch, aliases={}):
        return pl.pallas_call(
            body,
            in_specs=in_specs,
            out_specs=jax.tree.map(lambda _: vmem, out_shape),
            out_shape=out_shape,
            scratch_shapes=scratch,
            cost_estimate=cost,
            compiler_params=pltpu.CompilerParams(vmem_limit_bytes=14 << 20),
            input_output_aliases=aliases,
        )

    rows = n // peers
    lit = rows * n // 128
    basis, basis_t = (jnp.asarray(table) for table in transform_tables(n))
    small = (velocity_class.transpose(1, 0, 2), class_slowness[None], slowness_detail[0])
    whole = (fields_top, basis, basis_t, *small)
    table = jax.ShapeDtypeStruct((n, n), BF16)
    scratch = [pltpu.VMEM(a.shape, a.dtype) for a in small]
    scratch += [pltpu.VMEM((small[0].shape[0], small[0].shape[2]), jnp.int32)] + work
    scratch += [pltpu.VMEM((n, 2 * n), F32), pltpu.VMEM((2, n, n), BF16), pltpu.SemaphoreType.DMA((7,))]
    *tables, receiver_top, source = call(
        opening_body,
        [pl.BlockSpec(memory_space=pltpu.SMEM)] + [pl.BlockSpec(memory_space=pltpu.HBM)] * len(whole),
        [table] * 2 + [cells] * 4 + [field] * 2,
        scratch,
    )(angular_freq, *(pltpu.with_memory_space_constraint(a, pltpu.HBM) for a in whole))
    sent_source = passed_along(source, "depth", 1)
    receiver, image, illum = call(
        first_image_body, [vmem] * (2 + TABLES), [field, cells, cells], work
    )(receiver_top, source, *tables)
    rising = passed_along(up_state[0, 0], "depth", -1)
    parcel_shape = jax.ShapeDtypeStruct((peers, 2 * lit + 16, 128), BF16)
    for tick in range(1, TICKS):
        sent_receiver = passed_along(receiver, "depth", 1)
        last = tick + 1 == TICKS
        args = (sent_source, surface, illum, *tables) if last else (sent_source, surface, *tables)
        made = call(
            partial(last_source_body if last else later_body, tick),
            [vmem] * len(args),
            [field, parcel_shape] if last else [field],
            work,
        )(*args)
        source = made[0]
        args = (sent_receiver, surface, source, image)
        if not last:
            sent_source = passed_along(source, "depth", 1)
            args = (*args, illum, *tables)
            receiver, image, illum = call(
                partial(later_image_body, tick), [vmem] * len(args), [field, cells, cells], work
            )(*args)
    args = (made[1], rising, *args, *tables)
    parcel = call(
        partial(last_image_body, TICKS - 1),
        [vmem] * len(args),
        parcel_shape,
        work + [pltpu.VMEM((2, n, n), BF16)],
        {0: 0},
    )(*args)
    balanced = jax.ShapeDtypeStruct((peers, lit + 8, 128), BF16)
    balanced = call(balance_body, [vmem], balanced, [])(exchanged(parcel))
    part, risen = call(
        upward_body, [vmem] * (3 + TABLES), [jax.ShapeDtypeStruct((rows, n), BF16), field], work
    )(exchanged(balanced), rising, source, *tables)
    return (part[None], risen[None, None])


def solution(mesh):
    return jax.shard_map(
        per_device,
        mesh=mesh,
        in_specs=(
            P("depth", None, "freq", None, None, None),
            P(None, None, "freq", None, None, None),
            P("depth", "freq", None, None, None),
            P("freq"),
            P(),
            P("depth", None, None),
            P("depth", None, None),
        ),
        out_specs=(P("depth", "freq", None), P("depth", "freq", None, None, None)),
        check_vma=False,
    )
```

```python
from functools import partial

import jax
import jax.numpy as jnp
import ml_dtypes
import numpy as np
from jax import lax
from jax.experimental import pallas as pl
from jax.experimental.pallas import tpu as pltpu
from jax.sharding import PartitionSpec as P

TICKS = 3
BLOCK = 32
DEPTH_STEP = 1.0
EPSILON = 1e-06
F32 = jnp.float32
BF16 = jnp.bfloat16


def transform_tables(lateral):
    half = lateral // 2
    place = np.arange(lateral)
    wave = np.where(place <= half, place, place - half)
    angles = (place[:, None] * wave[None, :] % lateral) * (2.0 * np.pi / lateral)
    basis = np.where(place[None, :] <= half, np.cos(angles), np.sin(angles))
    basis = basis.astype(np.float32).astype(ml_dtypes.bfloat16)
    return basis, np.ascontiguousarray(basis.T)


def sincos(x):
    y = x * 0.25
    z = y * y
    s = y + y * z * (-1 / 6 + z * (1 / 120 + z * (-1 / 5040 + z * (1 / 362880 + z * (-1 / 39916800)))))
    c = 1.0 + z * (-1 / 2 + z * (1 / 24 + z * (-1 / 720 + z * (1 / 40320 + z * (-1 / 3628800 + z * (1 / 479001600))))))
    s2 = s * c
    s2 = s2 + s2
    c2 = 1.0 - 2.0 * (s * s)
    s4 = s2 * c2
    return s4 + s4, 1.0 - 2.0 * (s2 * s2)


def opening_body(angular, fields, basis_hbm, basis_t_hbm, classes_hbm, slow_hbm, detail_hbm,
                 basis, basis_t, phase_re, phase_im, lens_re, lens_im, receiver, out,
                 classes, class_slow, detail, kinds_of, wide, tall, spectrum, start, sems):
    pairs = (
        (fields.at[0, 0, 0], start),
        (basis_hbm, basis),
        (basis_t_hbm, basis_t),
        (classes_hbm, classes),
        (slow_hbm, class_slow),
        (detail_hbm, detail),
        (fields.at[0, 1, 0], receiver),
    )
    copies = [pltpu.make_async_copy(a, b, sems.at[k]) for k, (a, b) in enumerate(pairs)]
    for copy in copies:
        copy.start()
    for copy in copies[:3]:
        copy.wait()
    lateral = detail.shape[0]
    blocks = lateral // BLOCK
    half = lateral // 2
    step = 2.0 * np.pi / lateral
    lane_block = lax.broadcasted_iota(jnp.int32, (1, lateral), 1) // BLOCK

    def axis_terms(shape, dim, offset):
        place = lax.broadcasted_iota(jnp.int32, shape, dim) + offset
        wave = jnp.where(place <= half, place, place - half)
        kappa = wave.astype(F32) * step
        weight = jnp.where((wave == 0) | (wave == half), 1.0, 2.0)
        return kappa * kappa, weight

    lane_sq, lane_weight = axis_terms((1, lateral), 1, 0)
    for copy in copies[3:5]:
        copy.wait()
    for i in range(blocks):
        kinds_of[i : i + 1, :] = classes[i]
    kinds = kinds_of[...]
    slow = jnp.zeros(kinds.shape, F32)
    for kind in range(class_slow.shape[1]):
        slow = jnp.where(kinds == kind, class_slow[0:1, kind : kind + 1], slow)
    w = angular[0]
    spread = jnp.zeros((blocks, lateral), F32)
    for j in range(blocks):
        spread = jnp.where(lane_block == j, slow[:, j : j + 1], spread)
    copies[5].wait()
    total = jnp.zeros((8, lateral), F32)
    for i in range(blocks):
        cells = spread[i : i + 1, :] * detail[i * BLOCK : (i + 1) * BLOCK, :]
        lens_re[i * BLOCK : (i + 1) * BLOCK, :] = cells
        total = total + cells.reshape(BLOCK // 8, 8, lateral).sum(axis=0)
    mean = jnp.sum(jnp.sum(total, axis=0, keepdims=True), axis=1, keepdims=True) / (lateral * lateral)
    square = (w * mean) * (w * mean)
    scale = w * DEPTH_STEP

    def phases(start, rows):
        row_sq, row_weight = axis_terms((rows, 1), 0, start)
        vertical = square - (row_sq + lane_sq)
        root = jnp.sqrt(jnp.abs(vertical)) * DEPTH_STEP
        decay = jnp.where(vertical < 0.0, jnp.exp(-root), 1.0)
        decay = decay * (row_weight * lane_weight / (lateral * lateral))
        travel_sin, travel_cos = sincos(jnp.where(vertical > 0.0, root, 0.0))
        return decay * travel_cos, decay * travel_sin

    rows = 32

    spectrum[...] = to_spectrum(start[...].reshape(tall.shape), basis, basis_t, wide)
    for first in range(0, half, rows):
        real, imag = phases(first, rows)
        for here in (slice(first, first + rows), slice(half + first, half + first + rows)):
            phase_re[here, :] = real
            phase_im[here, :] = imag
    phase_re[half : half + 8, :], phase_im[half : half + 8, :] = phases(half, 8)
    for first in range(0, lateral, rows):
        here = slice(first, first + rows)
        lens_sin, lens_cos = sincos(scale * (lens_re[here, :] - mean))
        lens_re[here, :] = lens_cos
        lens_im[here, :] = lens_sin
    from_spectrum(
        spectrum[...], basis, basis_t, phase_re, phase_im, lens_re, lens_im, wide, tall, put(out)
    )
    copies[6].wait()


def step_core(start, basis, basis_t, phase_re, phase_im, lens_re, lens_im, wide, tall, write):
    spectrum = to_spectrum(start, basis, basis_t, wide)
    from_spectrum(spectrum, basis, basis_t, phase_re, phase_im, lens_re, lens_im, wide, tall, write)


def to_spectrum(start, basis, basis_t, wide):
    n = basis.shape[0]
    first = jnp.dot(start, basis[...], preferred_element_type=F32).astype(BF16)
    wide[:, :n] = first[:n]
    wide[:, n:] = first[n:]
    return jnp.dot(basis_t[...], wide[...], preferred_element_type=F32)


def from_spectrum(spectrum, basis, basis_t, phase_re, phase_im, lens_re, lens_im, wide, tall, write):
    n = basis.shape[0]
    spec_re, spec_im = spectrum[:, :n], spectrum[:, n:]
    wide[:, :n] = (spec_re * phase_re[...] - spec_im * phase_im[...]).astype(BF16)
    wide[:, n:] = (spec_re * phase_im[...] + spec_im * phase_re[...]).astype(BF16)
    back = jnp.dot(basis[...], wide[...], preferred_element_type=F32).astype(BF16)
    tall[:n, :] = back[:, :n]
    tall[n:, :] = back[:, n:]
    space = jnp.dot(tall[...], basis_t[...], preferred_element_type=F32)
    space_re, space_im = space[:n], space[n:]
    write(
        (space_re * lens_re[...] - space_im * lens_im[...]).astype(BF16),
        (space_re * lens_im[...] + space_im * lens_re[...]).astype(BF16),
    )


def entering(arrived, surface, tick, kind, tall):
    n = arrived.shape[-1]

    @pl.when(lax.axis_index("depth") == 0)
    def _():
        tall[...] = surface[tick - 1, kind, 0].reshape(2 * n, n)

    @pl.when(lax.axis_index("depth") != 0)
    def _():
        tall[...] = arrived[...].reshape(2 * n, n)

    return tall[...]


def put(out):
    def write(real, imag):
        out[0] = real
        out[1] = imag

    return write


TABLES = 6


def later_body(tick, arrived, surface, *refs):
    tables, (out, wide, tall) = refs[:TABLES], refs[TABLES:]
    step_core(entering(arrived, surface, tick, 0, tall), *tables, wide, tall, put(out))


def add_terms(source, receiver, image, illum):
    s_re, s_im = source[0].astype(F32), source[1].astype(F32)
    r_re, r_im = receiver[0].astype(F32), receiver[1].astype(F32)
    return image + (s_re * r_re + s_im * r_im), illum + (s_re * s_re + s_im * s_im)


def pieces(value, rows):
    high = value.astype(BF16).astype(F32)
    middle = (value - high).astype(BF16).astype(F32)
    low = value - high - middle
    row = lax.broadcasted_iota(jnp.int32, (rows, 128), 0)
    parts = jnp.where(row == 0, high, jnp.where(row == 1, middle, jnp.where(row == 2, low, 0.0)))
    return parts.astype(BF16)


def first_image_body(start, source, *refs):
    tables, (out, image, illum, wide, tall) = refs[:TABLES], refs[TABLES:]
    n = start.shape[-1]
    step_core(start[...].reshape(2 * n, n), *tables, wide, tall, put(out))
    image[...], illum[...] = add_terms(source, out, 0.0, 0.0)


def later_image_body(tick, arrived, surface, source, image_in, illum_in, *refs):
    tables, (out, image, illum, wide, tall) = refs[:TABLES], refs[TABLES:]
    step_core(entering(arrived, surface, tick, 1, tall), *tables, wide, tall, put(out))
    image[...], illum[...] = add_terms(source, out, image_in[...], illum_in[...])


def last_source_body(tick, arrived, surface, illum_in, *refs):
    tables, (out, parcel, wide, tall) = refs[:TABLES], refs[TABLES:]
    step_core(entering(arrived, surface, tick, 0, tall), *tables, wide, tall, put(out))
    peers = parcel.shape[0]
    n = illum_in.shape[0]
    rows = n // peers
    lit = 3 * rows
    total = jnp.zeros((rows, n), F32)
    for peer in range(peers):
        here = slice(peer * rows, (peer + 1) * rows)
        s_re, s_im = out[0, here, :].astype(F32), out[1, here, :].astype(F32)
        illum = illum_in[here, :] + (s_re * s_re + s_im * s_im)
        total = total + illum
        small = illum.astype(BF16)
        for lane in range(3):
            there = slice(lit + lane * rows, lit + (lane + 1) * rows)
            parcel[peer, there, :] = small[:, lane * 128 : (lane + 1) * 128]
    extra = pieces(jnp.sum(total), 16)
    for peer in range(peers):
        parcel[peer, 2 * lit : 2 * lit + 16, :] = extra
        parcel[peer, 0:lit, :] = jnp.zeros((lit, 128), BF16)


def last_image_body(tick, begun, rising, arrived, surface, source, image_in, *refs):
    tables, (parcel, wide, tall, out) = refs[:TABLES], refs[TABLES:]
    peers = parcel.shape[0]
    n = image_in.shape[0]
    rows = n // peers
    step_core(entering(arrived, surface, tick, 1, tall), *tables, wide, tall, put(out))
    for peer in range(peers):
        here = slice(peer * rows, (peer + 1) * rows)
        image = image_in[here, :]
        for part in range(2):
            image = image + source[part, here, :].astype(F32) * out[part, here, :].astype(F32)
        small = image.astype(BF16)
        for lane in range(3):
            parcel[peer, lane * rows : (lane + 1) * rows, :] = small[:, lane * 128 : (lane + 1) * 128]


def balance_body(parcel, out):
    peers, height, lanes = parcel.shape
    lit = (height - 16) // 2
    cells = lit * lanes * peers
    sums = parcel[0].astype(F32)
    for peer in range(1, peers):
        sums = sums + parcel[peer].astype(F32)
    image, illum = sums[:lit], sums[lit : 2 * lit]
    damping = jnp.sum(sums[2 * lit :, 0:1]) / cells
    balanced = image / (illum + damping)
    small = balanced.astype(BF16)
    extra = pieces(jnp.sum(balanced * balanced), 8)
    for peer in range(peers):
        out[peer, 0:lit, :] = small
        out[peer, lit : lit + 8, :] = extra


def upward_body(parcel, rising, source, *refs):
    tables, (part, out, wide, tall) = refs[:TABLES], refs[TABLES:]
    peers, _, lanes = parcel.shape
    n = source.shape[-1]
    rows = n // peers
    square = jnp.zeros((8, lanes), F32)
    for peer in range(peers):
        square = square + parcel[peer, 3 * rows : 3 * rows + 8, :].astype(F32)
    scale = lax.rsqrt(jnp.sum(square[:, 0:1]) / (n * n) + EPSILON)
    own = (parcel[pl.ds(lax.axis_index("freq"), 1)][0].astype(F32) * scale).astype(BF16)
    for lane in range(3):
        part[:, lane * lanes : (lane + 1) * lanes] = own[lane * rows : (lane + 1) * rows]
    for peer in range(peers):
        here = slice(peer * rows, (peer + 1) * rows)
        for lane in range(3):
            there = slice(lane * lanes, (lane + 1) * lanes)
            reflect = parcel[peer, lane * rows : (lane + 1) * rows, :].astype(F32) * scale
            reflect = reflect.astype(BF16).astype(F32)
            for half in range(2):
                lifted = rising[half, here, there].astype(F32) + reflect * source[half, here, there].astype(F32)
                tall[half * n + peer * rows : half * n + (peer + 1) * rows, there] = lifted.astype(BF16)
    step_core(tall[...], *tables, wide, tall, put(out))


def passed_along(block, axis, distance):
    devices = range(lax.axis_size(axis))
    route = [(i - distance, i) for i in devices if i - distance in devices]
    return lax.ppermute(block, axis, route)


def exchanged(parcel):
    return lax.all_to_all(parcel, "freq", split_axis=0, concat_axis=0, tiled=True)


def per_device(
    fields_top, surface, up_state, angular_freq, class_slowness, velocity_class, slowness_detail
):
    n = fields_top.shape[-1]
    peers = lax.axis_size("freq")
    vmem = pl.BlockSpec(memory_space=pltpu.VMEM)
    field = jax.ShapeDtypeStruct((2, n, n), BF16)
    cells = jax.ShapeDtypeStruct((n, n), F32)
    work = [pltpu.VMEM((n, 2 * n), BF16), pltpu.VMEM((2 * n, n), BF16)]
    cost = pl.CostEstimate(flops=2 * 4 * 2 * n**3, transcendentals=0, bytes_accessed=8 * n * n)

    def call(body, in_specs, out_shape, scratch, aliases={}):
        return pl.pallas_call(
            body,
            in_specs=in_specs,
            out_specs=jax.tree.map(lambda _: vmem, out_shape),
            out_shape=out_shape,
            scratch_shapes=scratch,
            cost_estimate=cost,
            compiler_params=pltpu.CompilerParams(vmem_limit_bytes=14 << 20),
            input_output_aliases=aliases,
        )

    rows = n // peers
    lit = rows * n // 128
    basis, basis_t = (jnp.asarray(table) for table in transform_tables(n))
    small = (velocity_class.transpose(1, 0, 2), class_slowness[None], slowness_detail[0])
    whole = (fields_top, basis, basis_t, *small)
    table = jax.ShapeDtypeStruct((n, n), BF16)
    scratch = [pltpu.VMEM(a.shape, a.dtype) for a in small]
    scratch += [pltpu.VMEM((small[0].shape[0], small[0].shape[2]), jnp.int32)] + work
    scratch += [pltpu.VMEM((n, 2 * n), F32), pltpu.VMEM((2, n, n), BF16), pltpu.SemaphoreType.DMA((7,))]
    *tables, receiver_top, source = call(
        opening_body,
        [pl.BlockSpec(memory_space=pltpu.SMEM)] + [pl.BlockSpec(memory_space=pltpu.HBM)] * len(whole),
        [table] * 2 + [cells] * 4 + [field] * 2,
        scratch,
    )(angular_freq, *(pltpu.with_memory_space_constraint(a, pltpu.HBM) for a in whole))
    sent_source = passed_along(source, "depth", 1)
    receiver, image, illum = call(
        first_image_body, [vmem] * (2 + TABLES), [field, cells, cells], work
    )(receiver_top, source, *tables)
    rising = passed_along(up_state[0, 0], "depth", -1)
    parcel_shape = jax.ShapeDtypeStruct((peers, 2 * lit + 16, 128), BF16)
    for tick in range(1, TICKS):
        sent_receiver = passed_along(receiver, "depth", 1)
        last = tick + 1 == TICKS
        args = (sent_source, surface, illum, *tables) if last else (sent_source, surface, *tables)
        made = call(
            partial(last_source_body if last else later_body, tick),
            [vmem] * len(args),
            [field, parcel_shape] if last else [field],
            work,
        )(*args)
        source = made[0]
        args = (sent_receiver, surface, source, image)
        if not last:
            sent_source = passed_along(source, "depth", 1)
            args = (*args, illum, *tables)
            receiver, image, illum = call(
                partial(later_image_body, tick), [vmem] * len(args), [field, cells, cells], work
            )(*args)
    args = (made[1], rising, *args, *tables)
    parcel = call(
        partial(last_image_body, TICKS - 1),
        [vmem] * len(args),
        parcel_shape,
        work + [pltpu.VMEM((2, n, n), BF16)],
        {0: 0},
    )(*args)
    balanced = jax.ShapeDtypeStruct((peers, lit + 8, 128), BF16)
    balanced = call(balance_body, [vmem], balanced, [])(exchanged(parcel))
    part, risen = call(
        upward_body, [vmem] * (3 + TABLES), [jax.ShapeDtypeStruct((rows, n), BF16), field], work
    )(exchanged(balanced), rising, source, *tables)
    return (part[None], risen[None, None])


def solution(mesh):
    return jax.shard_map(
        per_device,
        mesh=mesh,
        in_specs=(
            P("depth", None, "freq", None, None, None),
            P(None, None, "freq", None, None, None),
            P("depth", "freq", None, None, None),
            P("freq"),
            P(),
            P("depth", None, None),
            P("depth", None, None),
        ),
        out_specs=(P("depth", "freq", None), P("depth", "freq", None, None, None)),
        check_vma=False,
    )
```
